32 devices in a mesh: dev: 32 (over z, y, x, core).
Axes of the slice: x: 2, y: 2, z: 4, core: 2. Of those that a mesh axis runs over, the one named last changes fastest.
Arguments:
- table: bfloat16 [32768, 512], P('dev'), may hold values from -6 to 6
- owners: int32 [32768, 4], P('dev'), may hold values from 0 to 31, all different within a row; in each aligned block of 1024 rows (0 to 1023, 1024 to 2047, ...) at most 256 rows name the same one
- local_rows: int32 [32768, 4], P('dev'), may hold values from 0 to 1023
- segments: int32 [32, 1024], P('dev'), may hold values from 0 to 3, never falling along the last dimension, each value on 1 to 512 neighbouring positions
- cotangent: bfloat16 [32768, 512], P('dev'), may hold values from -6 to 6
- weights: bfloat16 [512, 2560], replicated, may hold values from -0.25 to 0.25
- master: float32 [512, 2560], P('dev'), may hold values from -0.25 to 0.25
- moment1: float32 [512, 2560], P('dev'), may hold values from -6 to 6
- moment2: float32 [512, 2560], P('dev'), may hold values from 0.2 to 5
Outputs:
- table_grad: float32 [32768, 512], P('dev')
- new_weights: bfloat16 [512, 2560], replicated
- new_master: float32 [512, 2560], P('dev')
- new_moment1: float32 [512, 2560], P('dev')
- new_moment2: float32 [512, 2560], P('dev')
The draws below stay inside these ranges and needn't reach their ends.
Inputs may be any that keep to these rules, and one draw needn't show every extreme that they name: Each history row names 4 different owners; within the 1024 rows of one device no owner is named more than 256 times, and that bound is reached on some devices. `segments`: within each row, sequence numbers never fall and each sequence holds 1 to 512 rows.
All inputs are finite; a program needn't handle non-finite values.
Results may differ from the reference program's by a relative error of at most 0.012.
Values may be sent and summed in bfloat16 or wider, within the bound.
No kernel may reach another device: no remote copies, remote signals or barrier semaphores. Data moves between devices by JAX's collectives and lax.ppermute only.
A program may use at most 320 MiB of HBM per device.

```python
import math
import jax
import jax.numpy as jnp
import numpy as np
from jax import lax

D = 512
HEADS = 8
FEATS = 4
MAXLEN = 512
TOK_DEV = 1024
ROWS_DEV = 1024
SEQ_DEV = 4
CAP = 256
TOKENS = 32768
TABLE = 32768
N_DEV = 32


def place_ends(entries, stream_key, low, high):
    longest = entries.shape.index(max(entries.shape))
    spots = []
    for shift in (0, 1):
        where = [jax.random.randint(jax.random.fold_in(stream_key, axis), (), 0, length) for axis, length in enumerate(entries.shape)]
        where[longest] = (where[longest] + shift) % entries.shape[longest]
        spots.append(tuple(where))
    return entries.at[spots[0]].set(low).at[spots[1]].set(high)


def steps_of(stream_key, extent, shards, least, high):
    gain = 1.0
    for axis_at, shards_of in shards:
        heights = jax.random.uniform(jax.random.fold_in(jax.random.fold_in(stream_key, 6), axis_at), (shards_of,), jnp.float32, least / len(shards), high / len(shards))
        gain = gain * jnp.repeat(jnp.exp(heights), extent[axis_at] // shards_of).reshape((-1,) + (1,) * (len(extent) - 1 - axis_at))
    return gain


def length_profile(amount, total, bound, lean):
    loads = [(1 << 20) // math.isqrt(standing ** lean) + 1 for standing in range(2, amount + 1)]
    rest, counts = total - bound - (amount - 1), [1] * (amount - 1)
    while rest > 0:
        free = [i for i in range(amount - 1) if counts[i] < bound]
        pool, budget = sum([loads[i] for i in free]), rest
        for i in free:
            addition = min(bound - counts[i], max(1, budget * loads[i] // pool), rest)
            counts[i] = counts[i] + addition
            rest = rest - addition
    return np.array([bound] + counts)


def ragged(stream_key, count, total, limit, lean):
    if count == 2:
        one = jax.random.randint(stream_key, (), max(1, total - limit), min(limit, total - 1) + 1)
        return jnp.stack([one, total - one])
    lengths = jnp.asarray(length_profile(count, total, limit, lean), jnp.int32)
    twos = (count - 1) // 2
    giver, taker = lengths[1:1 + 2 * twos:2], lengths[2:2 + 2 * twos:2]
    margin = jnp.minimum(giver - 1, limit - taker)
    passed = jax.random.randint(jax.random.fold_in(stream_key, 1), (twos,), 0, 1 << 20) % (margin + 1)
    lengths = lengths.at[1:1 + 2 * twos:2].set(giver - passed).at[2:2 + 2 * twos:2].set(taker + passed)
    return lengths[jax.random.permutation(jax.random.fold_in(stream_key, 2), count)]


def deal_out(stream_key, own, number, rows, amount, top, reach, lean):
    sequence = jax.random.permutation(stream_key, amount)
    packed, usual = shares(amount, rows * top, reach, lean, True), shares(amount, rows * top, reach, lean, False)
    places = jnp.arange(amount)

    def named(tallies, rotation):
        used = int((tallies > 0).sum())
        fixed = max(1, used // 4)
        moved = fixed + (places - fixed + rotation * (used - fixed)) % max(1, amount - fixed)
        return jnp.zeros((amount,), jnp.int32).at[sequence[jnp.where(places < fixed, places, moved)]].set(jnp.asarray(tallies, jnp.int32))

    tallies = jnp.where(number % 4 == 0, named(packed, number // 4), named(usual, number - number // 4 - 1))
    mixed = jax.random.permutation(jax.random.fold_in(own, 3), amount)
    giver, receiver = mixed[0:amount // 2 * 2:2], mixed[1:amount // 2 * 2:2]
    margin = jnp.minimum(tallies[giver] - 1, reach - tallies[receiver]) // 2
    margin = jnp.where((giver == sequence[0]) | (receiver == sequence[0]) | (tallies[receiver] == 0), 0, jnp.maximum(margin, 0))
    moved = jax.random.randint(jax.random.fold_in(own, 4), (amount // 2,), 0, 1 << 20) % (margin + 1)
    tallies = tallies.at[giver].add(-moved).at[receiver].add(moved)
    items = jnp.searchsorted(jnp.cumsum(tallies), jnp.arange(rows * top), side="right").astype(jnp.int32)
    table = items.reshape(top, rows).T
    table = table[jax.random.permutation(jax.random.fold_in(own, 1), rows)]
    rotation = jax.random.randint(jax.random.fold_in(own, 2), (rows, 1), 0, top)
    return jnp.take_along_axis(table, (jnp.arange(top)[None, :] + rotation) % top, axis=1)


def shares(number_of, total, most, slope, full):
    loads = [(1 << 20) // math.isqrt(standing ** slope) + 1 for standing in range(1, number_of + 1)]
    largest = most if full else min(most, max(-(-total // number_of), total * loads[0] // sum(loads)))
    least = 1 if total - largest >= number_of - 1 else 0
    given, spare = [largest] + [least] * (number_of - 1), total - largest - least * (number_of - 1)
    while spare > 0:
        candidates = [i for i in range(1, number_of) if given[i] < largest] or [i for i in range(1, number_of) if given[i] < most]
        pool, remaining = sum([loads[i] for i in candidates]), spare
        for i in candidates:
            more = min(most - given[i], max(1, remaining * loads[i] // pool), spare)
            given[i] = given[i] + more
            spare = spare - more
    return np.array(given)


def gaussian(key, shape, deviation, most, cuts=(), held_as=jnp.bfloat16):
    values = deviation * jax.random.normal(key, shape, jnp.float32)
    if cuts:
        values = values * steps_of(key, shape, cuts, -0.22, 0.18)
    return jnp.clip(values, -most, most).astype(held_as)


def setup_inputs(seed: int = 0) -> dict:
    key_list = jax.random.split(jax.random.key(seed), 10)
    table = gaussian(key_list[0], (TABLE, D), 1.0, 6.0, ((0, 32),))
    owners_keys = jax.random.split(jax.random.fold_in(key_list[1], 1), TOKENS // TOK_DEV)
    owners_turns = jax.random.permutation(jax.random.fold_in(key_list[1], 3), TOKENS // TOK_DEV)
    owners = jax.vmap(lambda own, number: deal_out(jax.random.fold_in(key_list[1], 2), own, number, TOK_DEV, N_DEV, FEATS, CAP, 2))(owners_keys, owners_turns).reshape((TOKENS, FEATS))
    local_rows = place_ends(jax.random.randint(key_list[2], (TOKENS, FEATS), 0, ROWS_DEV), jax.random.fold_in(key_list[2], 1), 0, ROWS_DEV - 1).astype(jnp.int32)
    segments = jax.vmap(lambda own: jnp.searchsorted(jnp.cumsum(ragged(own, SEQ_DEV, TOK_DEV, MAXLEN, 2)), jnp.arange(TOK_DEV), side="right"))(jax.random.split(key_list[3], N_DEV)).reshape((N_DEV, TOK_DEV)).astype(jnp.int32)
    cotangent = gaussian(key_list[4], (TOKENS, D), 1.0, 6.0, ((0, 32),))
    weights = gaussian(key_list[5], (D, 5 * D), D ** -0.5, 0.25)
    master = gaussian(key_list[6], (D, 5 * D), D ** -0.5, 0.25, ((0, 32),), jnp.float32)
    moment1 = gaussian(key_list[7], (D, 5 * D), 1.0, 6.0, ((0, 32),), jnp.float32)
    moment2 = jnp.clip(jnp.exp(math.log(5.0) - 3.218876 * jax.random.uniform(key_list[8], (D, 5 * D), jnp.float32) ** steps_of(key_list[8], (D, 5 * D), ((0, 32),), -0.2, 0.2)), 0.2, 5.0)
    return dict(table=table, owners=owners, local_rows=local_rows, segments=segments, cotangent=cotangent, weights=weights, master=master, moment1=moment1, moment2=moment2)


def layer_norm(values):
    mean = lax.optimization_barrier(jnp.mean(values, axis=-1, keepdims=True))
    centred = values - mean
    var = lax.optimization_barrier(jnp.mean(centred * centred, axis=-1, keepdims=True))
    return centred * lax.rsqrt(var + 1e-05)

def head_attention(query, key, value, mask):
    scores = jnp.dot(query, key.T, preferred_element_type=jnp.float32)
    weight_mat = (jnp.where(mask, jax.nn.silu(scores), 0.0) / MAXLEN).astype(jnp.bfloat16)
    return jnp.dot(weight_mat, value, preferred_element_type=jnp.float32)

def attention_core(pre, segs):
    act = jax.nn.silu(pre).astype(jnp.bfloat16)
    count = pre.shape[0]
    width = act.shape[1] // 4
    gate = act[:, 0:width]
    value = act[:, width:2 * width]
    query = act[:, 2 * width:3 * width]
    key = act[:, 3 * width:4 * width]

    def split_heads(array):
        return array.reshape(count, HEADS, width // HEADS).transpose(1, 0, 2)
    places = jnp.arange(count, dtype=jnp.int32)
    mask = (segs[:, None] == segs[None, :]) & (places[:, None] >= places[None, :])
    heads_out = lax.map(lambda trio: head_attention(trio[0], trio[1], trio[2], mask), (split_heads(query), split_heads(key), split_heads(value)))
    attended = heads_out.transpose(1, 0, 2).reshape(count, width)
    return (layer_norm(attended) * gate.astype(jnp.float32)).astype(jnp.bfloat16)

def backward_pieces(rows, segs, weights, cotangent):
    width = weights.shape[0]
    rows_f = rows.astype(jnp.float32)
    normed, norm_back = jax.vjp(layer_norm, rows_f)
    normed_b = normed.astype(jnp.bfloat16)
    w_input = weights[:, :4 * width]
    w_output = weights[:, 4 * width:]
    pre = jnp.dot(normed_b, w_input, preferred_element_type=jnp.float32)
    mixed, core_back = jax.vjp(lambda values: attention_core(values, segs), pre)
    d_mixed = jnp.dot(cotangent, w_output.T, preferred_element_type=jnp.float32).astype(jnp.bfloat16)
    d_pre = core_back(d_mixed)[0].astype(jnp.bfloat16)
    d_normed = jnp.dot(d_pre, w_input.T, preferred_element_type=jnp.float32)
    d_rows = (norm_back(d_normed)[0] + cotangent.astype(jnp.float32)).astype(jnp.bfloat16)
    return (normed_b, mixed, d_pre, d_rows)

def adam_update(grad, master, moment1, moment2):
    new_m1 = 0.9 * moment1 + 0.1 * grad
    new_m2 = 0.95 * moment2 + 0.05 * grad * grad
    fix1 = 1.0 - 0.9 ** 10
    fix2 = 1.0 - 0.95 ** 10
    new_master = master - 0.01 * (new_m1 / fix1) / (jnp.sqrt(new_m2 / fix2) + 1e-08)
    return (new_master, new_m1, new_m2)

def reference(table, owners, local_rows, segments, cotangent, weights, master, moment1, moment2):
    ids = (owners * ROWS_DEV + local_rows).astype(jnp.int32)
    rows_all = lax.optimization_barrier(jnp.sum(table[ids].astype(jnp.float32), axis=1)).astype(jnp.bfloat16)

    def one_block(grad, block):
        rows, segs, cot = block
        normed_b, mixed, d_pre, d_rows = backward_pieces(rows, segs, weights, cot)
        term = jnp.concatenate([jnp.dot(normed_b.T, d_pre, preferred_element_type=jnp.float32), jnp.dot(mixed.T, cot, preferred_element_type=jnp.float32)], axis=1)
        return (grad + term, d_rows)
    start = jnp.zeros((D, 5 * D), jnp.float32)
    grad, d_rows = lax.scan(one_block, start, (rows_all.reshape(N_DEV, TOK_DEV, D), segments, cotangent.reshape(N_DEV, TOK_DEV, D)))
    spread = jnp.broadcast_to(d_rows.reshape(TOKENS, 1, D), (TOKENS, FEATS, D)).reshape(TOKENS * FEATS, D)
    table_grad = jnp.zeros((TABLE, D), jnp.float32).at[ids.reshape(-1)].add(spread.astype(jnp.float32))
    new_master, new_m1, new_m2 = adam_update(grad, master, moment1, moment2)
    return (table_grad, new_master.astype(jnp.bfloat16), new_master, new_m1, new_m2)
```

```python
import functools
import jax
import jax.numpy as jnp
from jax import lax
from jax.experimental import pallas as pl
from jax.experimental.pallas import tpu as pltpu
from jax.sharding import PartitionSpec as P

HEADS = 8
MAXLEN = 512
F32 = jnp.float32
BF16 = jnp.bfloat16
LANES = 128


def sigmoid(v):
    return 0.5 * jnp.tanh(0.5 * v) + 0.5


def nt(a, b):
    return lax.dot_general(a, b, (((1,), (1,)), ((), ())), preferred_element_type=F32)


def nn(a, b):
    return jnp.dot(a, b, preferred_element_type=F32)


def row_stats(v):
    mean = jnp.mean(v, axis=-1, keepdims=True)
    cen = v - mean
    var = jnp.mean(cen * cen, axis=-1, keepdims=True)
    rstd = lax.rsqrt(var + 1e-05)
    return cen * rstd, rstd


def norm_grad(hat, rstd, dy):
    m1 = jnp.mean(dy, axis=-1, keepdims=True)
    m2 = jnp.mean(dy * hat, axis=-1, keepdims=True)
    return rstd * (dy - m1 - hat * m2)


def dense_body(block, splits, *refs):
    x_refs, (segc_ref, segr_ref, w_ref, cot_ref) = refs[:splits], refs[splits:splits + 4]
    dx_refs, refs = refs[splits + 4:2 * splits + 4], refs[2 * splits + 4:]
    (normed_ref, mixed_ref, dpre_ref, mask, dsil, act, dmix, att, datt, wsave, dsave, dvt, dkt) = refs
    rows, width = cot_ref.shape
    wide = width // splits
    head = width // HEADS
    lanes = 2 * head
    npair = HEADS // 2
    nblk = rows // block
    band = -(-MAXLEN // block)
    tiles = [(q, k) for q in range(nblk) for k in range(max(0, q - band), q + 1)]
    where = {t: i for i, t in enumerate(tiles)}

    def rs(i):
        return pl.ds(pl.multiple_of(i * block, block), block)

    def x_rows(r):
        return jnp.concatenate([v[r, :] for v in x_refs], axis=1).astype(F32)

    def first(i, c):
        r = rs(i)
        hat, _ = row_stats(x_rows(r))
        nb = hat.astype(BF16)
        normed_ref[r, :] = nb
        for j in range(4):
            cols = slice(j * width, (j + 1) * width)
            pre = nn(nb, w_ref[:, cols])
            sg = sigmoid(pre)
            a = pre * sg
            act[r, cols] = a.astype(BF16)
            dsil[r, cols] = sg + a * (1.0 - sg)
        dmix[r, :] = nt(cot_ref[r, :], w_ref[:, 4 * width:]).astype(BF16)
        return c

    lax.fori_loop(0, nblk, first, 0)

    for j, (q, k) in enumerate(tiles):
        same = segc_ref[q * block:(q + 1) * block, :] == segr_ref[:, k * block:(k + 1) * block]
        if q == k:
            ri = lax.broadcasted_iota(jnp.int32, (block, block), 0)
            ci = lax.broadcasted_iota(jnp.int32, (block, block), 1)
            same = same & (ri >= ci)
        mask[j] = jnp.where(same, 1.0 / MAXLEN, 0.0)

    low = lax.broadcasted_iota(jnp.int32, (block, lanes), 1) < head

    def halves(v):
        zero = jnp.zeros_like(v)
        return jnp.where(low, v, zero), jnp.where(low, zero, v)

    def cols(part, p):
        return pl.ds(pl.multiple_of(part * width + p * lanes, lanes), lanes)

    def forward(p, c):
        for q in range(nblk):
            qr = slice(q * block, (q + 1) * block)
            qh = halves(act[qr, cols(2, p)])
            acc = jnp.zeros((block, lanes), F32)
            for k in range(max(0, q - band), q + 1):
                kr = slice(k * block, (k + 1) * block)
                j = where[(q, k)]
                key = act[kr, cols(3, p)]
                vh = halves(act[kr, cols(1, p)])
                for h in range(2):
                    s = nt(qh[h], key)
                    m = mask[j]
                    sg = sigmoid(s)
                    a = s * sg
                    wt = (a * m).astype(BF16)
                    wsave[p * 2 + h, j] = wt
                    dsave[p * 2 + h, j] = ((sg + a * (1.0 - sg)) * m).astype(BF16)
                    acc += nn(wt, vh[h])
            att[qr, cols(0, p)] = acc
        return c

    lax.fori_loop(0, npair, forward, 0)

    def middle(i, c):
        r = rs(i)
        hat, rstd = row_stats(att[r, :])
        g = act[r, 0:width].astype(F32)
        dm = dmix[r, :].astype(F32)
        mixed_ref[r, :] = (hat * g).astype(BF16)
        dgate = (dm * hat).astype(BF16).astype(F32)
        dpre_ref[r, 0:width] = (dgate * dsil[r, 0:width]).astype(BF16)
        datt[r, :] = norm_grad(hat, rstd, dm * g).astype(BF16)
        return c

    lax.fori_loop(0, nblk, middle, 0)

    def backward(p, c):
        dvt[...] = jnp.zeros(dvt.shape, F32)
        dkt[...] = jnp.zeros(dkt.shape, F32)
        for q in range(nblk):
            qr = slice(q * block, (q + 1) * block)
            da = datt[qr, cols(0, p)]
            qv = act[qr, cols(2, p)]
            dh = halves(da)
            dat = da.astype(F32).T.astype(BF16)
            qt = qv.astype(F32).T.astype(BF16)
            acc = jnp.zeros((block, lanes), F32)
            for k in range(max(0, q - band), q + 1):
                kr = slice(k * block, (k + 1) * block)
                j = where[(q, k)]
                val = act[kr, cols(1, p)]
                kh = halves(act[kr, cols(3, p)])
                for h in range(2):
                    hr = slice(h * head, (h + 1) * head)
                    dw = nt(dh[h], val).astype(BF16).astype(F32)
                    ds = (dw * dsave[p * 2 + h, j].astype(F32)).astype(BF16)
                    acc += nn(ds, kh[h])
                    dvt[hr, kr] += nn(dat[hr, :], wsave[p * 2 + h, j])
                    dkt[hr, kr] += nn(qt[hr, :], ds)
            dq = acc.astype(BF16).astype(F32)
            dpre_ref[qr, cols(2, p)] = (dq * dsil[qr, cols(2, p)]).astype(BF16)
        for k in range(nblk):
            kr = slice(k * block, (k + 1) * block)
            dv = dvt[:, kr].T.astype(BF16).astype(F32)
            dk = dkt[:, kr].T.astype(BF16).astype(F32)
            dpre_ref[kr, cols(1, p)] = (dv * dsil[kr, cols(1, p)]).astype(BF16)
            dpre_ref[kr, cols(3, p)] = (dk * dsil[kr, cols(3, p)]).astype(BF16)
        return c

    lax.fori_loop(0, npair, backward, 0)

    def last(i, c):
        r = rs(i)
        hat, rstd = row_stats(x_rows(r))
        dn = nt(dpre_ref[r, :], w_ref[:, 0:4 * width])
        dx = norm_grad(hat, rstd, dn) + cot_ref[r, :].astype(F32)
        for n, ref in enumerate(dx_refs):
            ref[r, :] = dx[:, n * wide:(n + 1) * wide].astype(BF16)
        return c

    lax.fori_loop(0, nblk, last, 0)


def dense(x, segs, weights, cot):
    splits = len(x)
    rows, width = cot.shape
    block = min(256, rows)
    nblk = rows // block
    band = -(-MAXLEN // block)
    ntile = sum(min(q, band) + 1 for q in range(nblk))
    lanes = 2 * width // HEADS
    vm = pl.BlockSpec(memory_space=pltpu.VMEM)
    return pl.pallas_call(
        functools.partial(dense_body, block, splits),
        out_shape=(jax.ShapeDtypeStruct((rows, width // splits), BF16),) * splits
        + (
            jax.ShapeDtypeStruct((rows, width), BF16),
            jax.ShapeDtypeStruct((rows, width), BF16),
            jax.ShapeDtypeStruct((rows, 4 * width), BF16),
        ),
        in_specs=[vm] * (splits + 4),
        out_specs=(vm,) * (splits + 3),
        scratch_shapes=[
            pltpu.VMEM((ntile, block, block), F32),
            pltpu.VMEM((rows, 4 * width), F32),
            pltpu.VMEM((rows, 4 * width), BF16),
            pltpu.VMEM((rows, width), BF16),
            pltpu.VMEM((rows, width), F32),
            pltpu.VMEM((rows, width), BF16),
            pltpu.VMEM((HEADS, ntile, block, block), BF16),
            pltpu.VMEM((HEADS, ntile, block, block), BF16),
            pltpu.VMEM((lanes, rows), F32),
            pltpu.VMEM((lanes, rows), F32),
        ],
        compiler_params=pltpu.CompilerParams(vmem_limit_bytes=60 * 1024 * 1024),
        name="dense_step",
    )(*x, segs.reshape(rows, 1), segs.reshape(1, rows), weights, cot)


def spread_rows(dst, base, src, chunk):
    rows, width = src.shape
    parts = width // LANES

    def step(i, c):
        for j in range(parts):
            piece = src[pl.ds(pl.multiple_of(i * chunk, chunk), chunk), j * LANES:(j + 1) * LANES]
            start = pl.multiple_of(base * parts + i * (chunk * parts), 8) + j
            dst[pl.ds(start, chunk, stride=parts), :] = piece.astype(F32)
        return c

    lax.fori_loop(0, rows // chunk, step, 0)


def join_rows(dst, src, base, chunk):
    rows, width = dst.shape
    parts = width // LANES

    def step(i, c):
        for j in range(parts):
            start = pl.multiple_of(base * parts + i * (chunk * parts), 8) + j
            piece = src[pl.ds(start, chunk, stride=parts), :]
            dst[pl.ds(pl.multiple_of(i * chunk, chunk), chunk), j * LANES:(j + 1) * LANES] = piece.astype(dst.dtype)
        return c

    lax.fori_loop(0, rows // chunk, step, 0)


def gather_body(ntab, unroll, idx, *refs):
    tabs, out, tab, acc = refs[:ntab], refs[ntab], refs[ntab + 1], refs[ntab + 2]
    rows, width = tabs[0].shape
    parts = width // LANES
    count = out.shape[0]
    feats = idx.shape[0] // count
    chunk = 64
    for i in range(ntab):
        spread_rows(tab, i * rows, tabs[i], chunk)
    tab[pl.ds(ntab * rows * parts, 8), :] = jnp.zeros((8, LANES), F32)

    def step(i, c):
        for u in range(unroll):
            t = i * unroll + u
            total = tab[pl.ds(idx[t], parts), :]
            for f in range(1, feats):
                total = total + tab[pl.ds(idx[f * count + t], parts), :]
            acc[pl.ds(t * parts, parts), :] = total
        return c

    lax.fori_loop(0, count // unroll, step, 0)
    join_rows(out, acc, 0, chunk)


def gather_sum(idx, tabs, dtype, count):
    rows, width = tabs[0].shape
    parts = width // LANES
    vm = pl.BlockSpec(memory_space=pltpu.VMEM)
    return pl.pallas_call(
        functools.partial(gather_body, len(tabs), 8),
        out_shape=jax.ShapeDtypeStruct((count, width), dtype),
        in_specs=[pl.BlockSpec(memory_space=pltpu.SMEM)] + [vm] * len(tabs),
        out_specs=vm,
        scratch_shapes=[
            pltpu.VMEM((len(tabs) * rows * parts + 8, LANES), F32),
            pltpu.VMEM((count * parts, LANES), F32),
        ],
        compiler_params=pltpu.CompilerParams(vmem_limit_bytes=60 * 1024 * 1024),
        name="gather_sum",
    )(idx, *tabs)


def scatter_body(npiece, nout, unroll, idx, *refs):
    pieces, outs, acc, stage = refs[:npiece], refs[npiece:npiece + nout], refs[-2], refs[-1]
    count, width = pieces[0].shape
    rows = outs[0].shape[0]
    parts = width // LANES
    feats = idx.shape[0] // (npiece * count)
    chunk = 64

    def clear(i, c):
        acc[pl.ds(pl.multiple_of(i * 256, 256), 256), :] = jnp.zeros((256, LANES), F32)
        return c

    lax.fori_loop(0, nout * rows * parts // 256, clear, 0)
    acc[pl.ds(nout * rows * parts, parts * feats), :] = jnp.zeros((parts * feats, LANES), F32)
    for n in range(npiece):
        spread_rows(stage, 0, pieces[n], chunk)

        def step(i, c):
            for u in range(unroll):
                t = i * unroll + u
                val = stage[pl.ds(t * parts, parts), :]
                at = [idx[(n * feats + f) * count + t] for f in range(feats)]
                got = [acc[pl.ds(a, parts), :] for a in at]
                for a, g in zip(at, got):
                    acc[pl.ds(a, parts), :] = g + val
            return c

        lax.fori_loop(0, count // unroll, step, 0)
    for o in range(nout):
        join_rows(outs[o], acc, o * rows, chunk)


def scatter_add(idx, pieces, nout, rows, dtypes):
    count, width = pieces[0].shape
    feats = idx.shape[0] // (len(pieces) * count)
    parts = width // LANES
    vm = pl.BlockSpec(memory_space=pltpu.VMEM)
    return pl.pallas_call(
        functools.partial(scatter_body, len(pieces), nout, 4),
        out_shape=tuple(jax.ShapeDtypeStruct((rows, width), d) for d in dtypes),
        in_specs=[pl.BlockSpec(memory_space=pltpu.SMEM)] + [vm] * len(pieces),
        out_specs=(vm,) * nout,
        scratch_shapes=[
            pltpu.VMEM(((nout * rows + feats) * parts, LANES), F32),
            pltpu.VMEM((count * parts, LANES), F32),
        ],
        compiler_params=pltpu.CompilerParams(vmem_limit_bytes=60 * 1024 * 1024),
        name="scatter_add",
    )(idx, *pieces)


SPLITS = 2
GROUP_BYTES = 16 * 1024 * 1024


def swap(v, bits):
    devices = lax.axis_size("dev")
    return lax.ppermute(v, "dev", [(i, i ^ bits) for i in range(devices)])


def sum_grad(grad, me, devices, block_rows):
    bits = devices.bit_length() - 1
    v = grad.reshape((2,) * bits + (block_rows, grad.shape[1]))
    for b in range(bits):
        axis = bits - 1 - b
        mine = (me >> b) & 1
        keep = lax.dynamic_index_in_dim(v, mine, axis, keepdims=False)
        give = lax.dynamic_index_in_dim(v, 1 - mine, axis, keepdims=False)
        v = keep + swap(give.astype(BF16), 1 << b).astype(F32)
    return v


def share_weights(v, me, devices):
    bits = devices.bit_length() - 1
    v = v[None]
    for b in reversed(range(bits)):
        got = swap(v, 1 << b)
        high = ((me >> b) & 1) == 1
        low_half = jnp.where(high, got, v)
        high_half = jnp.where(high, v, got)
        v = jnp.stack([low_half, high_half], axis=1).reshape((-1,) + v.shape[1:])
    return v


def shards(table, owners, local_rows, segments, cotangent, weights, master, moment1, moment2):
    devices = lax.axis_size("dev")
    me = lax.axis_index("dev")
    count, feats = owners.shape
    rows, width = table.shape
    wide = width // SPLITS
    parts = wide // LANES
    group = 1
    while group < devices and 2 * group * rows * width * 4 <= GROUP_BYTES:
        group *= 2
    columns = devices // group
    in_group = me % group
    column = me // group

    ids = (owners * rows + local_rows).T
    all_ids = [ids] + [swap(ids, k * group) for k in range(1, columns)]

    def places(v, spare):
        owner = v // rows
        place = ((owner % group) ^ in_group) * rows + v % rows
        return jnp.where(owner // group == column, place, spare) * parts

    x = []
    tabs = []
    for n in range(SPLITS):
        t = [None] * group
        t[0] = table[:, n * wide:(n + 1) * wide]
        for m in range(2, group, 2):
            t[m] = swap(t[0], m)
        tabs.append(t)
    sums = None
    for n in range(SPLITS):
        t = tabs[n]
        if sums is not None:
            sums, t = lax.optimization_barrier((sums, t))
        for m in range(0, group, 2):
            t[m + 1] = swap(t[m], 1)
        sums = [None] * columns
        for k in reversed(range(columns)):
            index = places(all_ids[k], group * rows).reshape(-1)
            sums[k] = gather_sum(index, t, BF16 if k else F32, count)
        total = sums[0]
        for k in range(1, columns):
            total = total + swap(sums[k], k * group).astype(F32)
        x.append(total.astype(BF16))

    out = dense(x, segments[0], weights, cotangent)
    dx, (normed, mixed, d_pre) = out[:SPLITS], out[SPLITS:]

    spare = group * rows + jnp.arange(feats, dtype=jnp.int32)[:, None]
    index = jnp.stack([places(v, spare) for v in all_ids]).reshape(-1)
    halves = []
    for n in range(SPLITS):
        pieces = [dx[n]] + [swap(dx[n], k * group) for k in range(1, columns)]
        outs = scatter_add(index, pieces, group, rows, (F32,) + (BF16,) * (group - 1))
        merged = []
        for m in range(0, group, 2):
            merged.append(outs[m].astype(F32) + swap(outs[m + 1], 1).astype(F32))
        total = merged[0]
        for i, m in enumerate(range(2, group, 2)):
            total = total + swap(merged[i + 1].astype(BF16), m).astype(F32)
        halves.append(total)
    table_grad = jnp.concatenate(halves, axis=1)

    grad_in = jnp.dot(normed.T, d_pre, preferred_element_type=F32)
    grad_out = jnp.dot(mixed.T, cotangent, preferred_element_type=F32)
    full_grad = jnp.concatenate([grad_in, grad_out], axis=1)
    grad = sum_grad(full_grad, me, devices, master.shape[0])
    new_m1 = 0.9 * moment1 + 0.1 * grad
    new_m2 = 0.95 * moment2 + 0.05 * grad * grad
    fix1 = 1.0 - 0.9**10
    fix2 = 1.0 - 0.95**10
    new_master = master - 0.01 * (new_m1 / fix1) / (jnp.sqrt(new_m2 / fix2) + 1e-08)
    new_weights = share_weights(new_master.astype(BF16), me, devices).reshape(weights.shape)
    return (table_grad, new_weights, new_master, new_m1, new_m2)


def solution(mesh):
    split = P("dev", None)
    return jax.shard_map(
        shards,
        mesh=mesh,
        in_specs=(split,) * 5 + (P(),) + (split,) * 3,
        out_specs=(split, P()) + (split,) * 3,
        check_vma=False,
    )
```

```python
import functools
import jax
import jax.numpy as jnp
from jax import lax
from jax.experimental import pallas as pl
from jax.experimental.pallas import tpu as pltpu
from jax.sharding import PartitionSpec as P

HEADS = 8
MAXLEN = 512
F32 = jnp.float32
BF16 = jnp.bfloat16
LANES = 128


def sigmoid(v):
    return 0.5 * jnp.tanh(0.5 * v) + 0.5


def nt(a, b):
    return lax.dot_general(a, b, (((1,), (1,)), ((), ())), preferred_element_type=F32)


def nn(a, b):
    return jnp.dot(a, b, preferred_element_type=F32)


def row_stats(v):
    mean = jnp.mean(v, axis=-1, keepdims=True)
    cen = v - mean
    var = jnp.mean(cen * cen, axis=-1, keepdims=True)
    rstd = lax.rsqrt(var + 1e-05)
    return cen * rstd, rstd


def norm_grad(hat, rstd, dy):
    m1 = jnp.mean(dy, axis=-1, keepdims=True)
    m2 = jnp.mean(dy * hat, axis=-1, keepdims=True)
    return rstd * (dy - m1 - hat * m2)


def dense_body(block, splits, *refs):
    x_refs, (segc_ref, segr_ref, w_ref, cot_ref) = refs[:splits], refs[splits:splits + 4]
    dx_refs, refs = refs[splits + 4:2 * splits + 4], refs[2 * splits + 4:]
    (normed_ref, mixed_ref, dpre_ref, mask, dsil, act, dmix, att, datt, wsave, dsave, dvt, dkt) = refs
    rows, width = cot_ref.shape
    wide = width // splits
    head = width // HEADS
    lanes = 2 * head
    npair = HEADS // 2
    nblk = rows // block
    band = -(-MAXLEN // block)
    tiles = [(q, k) for q in range(nblk) for k in range(max(0, q - band), q + 1)]
    where = {t: i for i, t in enumerate(tiles)}

    def rs(i):
        return pl.ds(pl.multiple_of(i * block, block), block)

    def x_rows(r):
        return jnp.concatenate([v[r, :] for v in x_refs], axis=1).astype(F32)

    def first(i, c):
        r = rs(i)
        hat, _ = row_stats(x_rows(r))
        nb = hat.astype(BF16)
        normed_ref[r, :] = nb
        for j in range(4):
            cols = slice(j * width, (j + 1) * width)
            pre = nn(nb, w_ref[:, cols])
            sg = sigmoid(pre)
            a = pre * sg
            act[r, cols] = a.astype(BF16)
            dsil[r, cols] = sg + a * (1.0 - sg)
        dmix[r, :] = nt(cot_ref[r, :], w_ref[:, 4 * width:]).astype(BF16)
        return c

    lax.fori_loop(0, nblk, first, 0)

    for j, (q, k) in enumerate(tiles):
        same = segc_ref[q * block:(q + 1) * block, :] == segr_ref[:, k * block:(k + 1) * block]
        if q == k:
            ri = lax.broadcasted_iota(jnp.int32, (block, block), 0)
            ci = lax.broadcasted_iota(jnp.int32, (block, block), 1)
            same = same & (ri >= ci)
        mask[j] = jnp.where(same, 1.0 / MAXLEN, 0.0)

    low = lax.broadcasted_iota(jnp.int32, (block, lanes), 1) < head

    def halves(v):
        zero = jnp.zeros_like(v)
        return jnp.where(low, v, zero), jnp.where(low, zero, v)

    def cols(part, p):
        return pl.ds(pl.multiple_of(part * width + p * lanes, lanes), lanes)

    def forward(p, c):
        for q in range(nblk):
            qr = slice(q * block, (q + 1) * block)
            qh = halves(act[qr, cols(2, p)])
            acc = jnp.zeros((block, lanes), F32)
            for k in range(max(0, q - band), q + 1):
                kr = slice(k * block, (k + 1) * block)
                j = where[(q, k)]
                key = act[kr, cols(3, p)]
                vh = halves(act[kr, cols(1, p)])
                for h in range(2):
                    s = nt(qh[h], key)
                    m = mask[j]
                    sg = sigmoid(s)
                    a = s * sg
                    wt = (a * m).astype(BF16)
                    wsave[p * 2 + h, j] = wt
                    dsave[p * 2 + h, j] = ((sg + a * (1.0 - sg)) * m).astype(BF16)
                    acc += nn(wt, vh[h])
            att[qr, cols(0, p)] = acc
        return c

    lax.fori_loop(0, npair, forward, 0)

    def middle(i, c):
        r = rs(i)
        hat, rstd = row_stats(att[r, :])
        g = act[r, 0:width].astype(F32)
        dm = dmix[r, :].astype(F32)
        mixed_ref[r, :] = (hat * g).astype(BF16)
        dgate = (dm * hat).astype(BF16).astype(F32)
        dpre_ref[r, 0:width] = (dgate * dsil[r, 0:width]).astype(BF16)
        datt[r, :] = norm_grad(hat, rstd, dm * g).astype(BF16)
        return c

    lax.fori_loop(0, nblk, middle, 0)

    def backward(p, c):
        dvt[...] = jnp.zeros(dvt.shape, F32)
        dkt[...] = jnp.zeros(dkt.shape, F32)
        for q in range(nblk):
            qr = slice(q * block, (q + 1) * block)
            da = datt[qr, cols(0, p)]
            qv = act[qr, cols(2, p)]
            dh = halves(da)
            dat = da.astype(F32).T.astype(BF16)
            qt = qv.astype(F32).T.astype(BF16)
            acc = jnp.zeros((block, lanes), F32)
            for k in range(max(0, q - band), q + 1):
                kr = slice(k * block, (k + 1) * block)
                j = where[(q, k)]
                val = act[kr, cols(1, p)]
                kh = halves(act[kr, cols(3, p)])
                for h in range(2):
                    hr = slice(h * head, (h + 1) * head)
                    dw = nt(dh[h], val).astype(BF16).astype(F32)
                    ds = (dw * dsave[p * 2 + h, j].astype(F32)).astype(BF16)
                    acc += nn(ds, kh[h])
                    dvt[hr, kr] += nn(dat[hr, :], wsave[p * 2 + h, j])
                    dkt[hr, kr] += nn(qt[hr, :], ds)
            dq = acc.astype(BF16).astype(F32)
            dpre_ref[qr, cols(2, p)] = (dq * dsil[qr, cols(2, p)]).astype(BF16)
        for k in range(nblk):
            kr = slice(k * block, (k + 1) * block)
            dv = dvt[:, kr].T.astype(BF16).astype(F32)
            dk = dkt[:, kr].T.astype(BF16).astype(F32)
            dpre_ref[kr, cols(1, p)] = (dv * dsil[kr, cols(1, p)]).astype(BF16)
            dpre_ref[kr, cols(3, p)] = (dk * dsil[kr, cols(3, p)]).astype(BF16)
        return c

    lax.fori_loop(0, npair, backward, 0)

    def last(i, c):
        r = rs(i)
        hat, rstd = row_stats(x_rows(r))
        dn = nt(dpre_ref[r, :], w_ref[:, 0:4 * width])
        dx = norm_grad(hat, rstd, dn) + cot_ref[r, :].astype(F32)
        for n, ref in enumerate(dx_refs):
            ref[r, :] = dx[:, n * wide:(n + 1) * wide].astype(BF16)
        return c

    lax.fori_loop(0, nblk, last, 0)


def dense(x, segs, weights, cot):
    splits = len(x)
    rows, width = cot.shape
    block = min(256, rows)
    nblk = rows // block
    band = -(-MAXLEN // block)
    ntile = sum(min(q, band) + 1 for q in range(nblk))
    lanes = 2 * width // HEADS
    vm = pl.BlockSpec(memory_space=pltpu.VMEM)
    return pl.pallas_call(
        functools.partial(dense_body, block, splits),
        out_shape=(jax.ShapeDtypeStruct((rows, width // splits), BF16),) * splits
        + (
            jax.ShapeDtypeStruct((rows, width), BF16),
            jax.ShapeDtypeStruct((rows, width), BF16),
            jax.ShapeDtypeStruct((rows, 4 * width), BF16),
        ),
        in_specs=[vm] * (splits + 4),
        out_specs=(vm,) * (splits + 3),
        scratch_shapes=[
            pltpu.VMEM((ntile, block, block), F32),
            pltpu.VMEM((rows, 4 * width), F32),
            pltpu.VMEM((rows, 4 * width), BF16),
            pltpu.VMEM((rows, width), BF16),
            pltpu.VMEM((rows, width), F32),
            pltpu.VMEM((rows, width), BF16),
            pltpu.VMEM((HEADS, ntile, block, block), BF16),
            pltpu.VMEM((HEADS, ntile, block, block), BF16),
            pltpu.VMEM((lanes, rows), F32),
            pltpu.VMEM((lanes, rows), F32),
        ],
        compiler_params=pltpu.CompilerParams(vmem_limit_bytes=60 * 1024 * 1024),
        name="dense_step",
    )(*x, segs.reshape(rows, 1), segs.reshape(1, rows), weights, cot)


def spread_rows(dst, base, src, chunk):
    rows, width = src.shape
    parts = width // LANES

    def step(i, c):
        for j in range(parts):
            piece = src[pl.ds(pl.multiple_of(i * chunk, chunk), chunk), j * LANES:(j + 1) * LANES]
            start = pl.multiple_of(base * parts + i * (chunk * parts), 8) + j
            dst[pl.ds(start, chunk, stride=parts), :] = piece.astype(F32)
        return c

    lax.fori_loop(0, rows // chunk, step, 0)


def join_rows(dst, srcs, base, chunk):
    rows, width = dst.shape
    parts = width // LANES

    def step(i, c):
        for j in range(parts):
            start = pl.multiple_of(base * parts + i * (chunk * parts), 8) + j
            piece = srcs[0][pl.ds(start, chunk, stride=parts), :]
            for src in srcs[1:]:
                piece = piece + src[pl.ds(start, chunk, stride=parts), :]
            dst[pl.ds(pl.multiple_of(i * chunk, chunk), chunk), j * LANES:(j + 1) * LANES] = piece.astype(dst.dtype)
        return c

    lax.fori_loop(0, rows // chunk, step, 0)


def gather_body(ntab, nout, unroll, idx, *refs):
    tabs, outs, tab, acc = refs[:ntab], refs[ntab:ntab + nout], refs[-2], refs[-1]
    rows, width = tabs[0].shape
    parts = width // LANES
    count = outs[0].shape[0]
    feats = idx.shape[0] // (count * nout)
    chunk = 64
    for i in range(ntab):
        spread_rows(tab, i * rows, tabs[i], chunk)
    tab[pl.ds(ntab * rows * parts, 8), :] = jnp.zeros((8, LANES), F32)
    for n, out in enumerate(outs):

        def step(i, c):
            for u in range(unroll):
                t = i * unroll + u
                total = tab[pl.ds(idx[n * feats * count + t], parts), :]
                for f in range(1, feats):
                    total = total + tab[pl.ds(idx[(n * feats + f) * count + t], parts), :]
                acc[pl.ds(t * parts, parts), :] = total
            return c

        lax.fori_loop(0, count // unroll, step, 0)
        join_rows(out, [acc], 0, chunk)


def gather_sum(idx, tabs, dtypes, count):
    rows, width = tabs[0].shape
    parts = width // LANES
    vm = pl.BlockSpec(memory_space=pltpu.VMEM)
    return pl.pallas_call(
        functools.partial(gather_body, len(tabs), len(dtypes), 8),
        out_shape=tuple(jax.ShapeDtypeStruct((count, width), d) for d in dtypes),
        in_specs=[pl.BlockSpec(memory_space=pltpu.SMEM)] + [vm] * len(tabs),
        out_specs=(vm,) * len(dtypes),
        scratch_shapes=[
            pltpu.VMEM((len(tabs) * rows * parts + 8, LANES), F32),
            pltpu.VMEM((count * parts, LANES), F32),
        ],
        compiler_params=pltpu.CompilerParams(vmem_limit_bytes=60 * 1024 * 1024),
        name="gather_sum",
    )(idx, *tabs)


def scatter_body(npiece, nout, lots, idx, *refs):
    pieces, outs = refs[:npiece], refs[npiece:npiece + nout]
    accs, stage = refs[npiece + nout:-1], refs[-1]
    count, width = pieces[0].shape
    rows = outs[0].shape[0]
    parts = width // LANES
    feats = idx.shape[0] // (npiece * count)
    chunk = 64

    def clear(i, c):
        for acc in accs:
            acc[pl.ds(pl.multiple_of(i * 256, 256), 256), :] = jnp.zeros((256, LANES), F32)
        return c

    lax.fori_loop(0, nout * rows * parts // 256, clear, 0)
    for acc in accs:
        acc[pl.ds(nout * rows * parts, parts * feats), :] = jnp.zeros((parts * feats, LANES), F32)
    for n in range(npiece):
        spread_rows(stage, 0, pieces[n], chunk)

        def step(i, c):
            for w in range(2):
                base = (i * 2 + w) * lots
                todo = []
                for u, acc in enumerate(accs):
                    val = stage[pl.ds((base + u) * parts, parts), :]
                    for f in range(feats):
                        at = idx[(n * feats + f) * count + base + u]
                        todo.append((acc, at, acc[pl.ds(at, parts), :] + val))
                for acc, at, val in todo:
                    acc[pl.ds(at, parts), :] = val
            return c

        lax.fori_loop(0, count // (2 * lots), step, 0)
    for o in range(nout):
        join_rows(outs[o], accs, o * rows, chunk)


def scatter_add(idx, pieces, nout, rows, dtypes):
    count, width = pieces[0].shape
    feats = idx.shape[0] // (len(pieces) * count)
    parts = width // LANES
    lots = 4
    vm = pl.BlockSpec(memory_space=pltpu.VMEM)
    return pl.pallas_call(
        functools.partial(scatter_body, len(pieces), nout, lots),
        out_shape=tuple(jax.ShapeDtypeStruct((rows, width), d) for d in dtypes),
        in_specs=[pl.BlockSpec(memory_space=pltpu.SMEM)] + [vm] * len(pieces),
        out_specs=(vm,) * nout,
        scratch_shapes=[pltpu.VMEM(((nout * rows + feats) * parts, LANES), F32)] * lots
        + [pltpu.VMEM((count * parts, LANES), F32)],
        compiler_params=pltpu.CompilerParams(vmem_limit_bytes=60 * 1024 * 1024),
        name="scatter_add",
    )(idx, *pieces)


def place_body(parts, at, *refs):
    blocks, out = refs[:-1], refs[-1]
    cols = blocks[0].shape[0]
    me = at[0]
    for core in range(2):
        for m in range(parts):
            ref = blocks[core * parts + m]
            for j in range(cols):
                out[(j * parts + m) * 2 + core ^ me] = ref[j]


def place_blocks(me, blocks):
    cols = blocks[0].shape[0]
    shape = (len(blocks) * cols,) + blocks[0].shape[1:]
    vm = pl.BlockSpec(memory_space=pltpu.VMEM)
    return pl.pallas_call(
        functools.partial(place_body, len(blocks) // 2),
        out_shape=jax.ShapeDtypeStruct(shape, blocks[0].dtype),
        in_specs=[pl.BlockSpec(memory_space=pltpu.SMEM)] + [vm] * len(blocks),
        out_specs=vm,
        name="place_blocks",
    )(me.reshape(1), *blocks)


SPLITS = 2
GROUP_BYTES = 16 * 1024 * 1024


def swap(v, bits):
    devices = lax.axis_size("dev")
    return lax.ppermute(v, "dev", [(i, i ^ bits) for i in range(devices)])


def gather_blocks(v, count, unit, direct):
    got = [v] + [None] * (count - 1)
    for k in range(1, count):
        mate = k % 2 and k > 1 and not direct
        got[k] = swap(got[k - 1], unit) if mate else swap(v, k * unit)
    return got


def merge_mates(outs, unit):
    merged = []
    for k in range(0, len(outs), 2):
        merged.append(outs[k].astype(F32) + swap(outs[k + 1], unit).astype(F32))
    return merged


def reduce_blocks(outs, unit):
    merged = merge_mates(outs, unit)
    total = merged[0]
    for i in range(1, len(merged)):
        total = total + swap(merged[i].astype(BF16), 2 * i * unit).astype(F32)
    return total


def pick(v, at, axis):
    return lax.dynamic_index_in_dim(v, at, axis, keepdims=False)


def sum_grad(grad, me, group, columns, block_rows):
    half = group // 2
    v = grad.reshape(columns, half, 2, block_rows, grad.shape[1])
    core, chip, column = me % 2, me // 2 % half, me // group
    v = pick(v, core, 2) + swap(pick(v, 1 - core, 2).astype(BF16), 1).astype(F32)
    total = pick(v, chip, 1)
    for m in range(1, half):
        total = total + swap(pick(v, chip ^ m, 1).astype(BF16), 2 * m).astype(F32)
    v = total
    total = pick(v, column, 0)
    for k in range(1, columns):
        total = total + swap(pick(v, column ^ k, 0).astype(BF16), k * group).astype(F32)
    return total


def share_weights(v, me, group, columns):
    half = group // 2
    v = jnp.stack([v] + [swap(v, k * group) for k in range(1, columns)])
    near = [v] + [swap(v, 2 * m) for m in range(1, half)]
    far = [swap(n, 1) for n in near]
    return place_blocks(me, near + far)


def shards(table, owners, local_rows, segments, cotangent, weights, master, moment1, moment2):
    devices = lax.axis_size("dev")
    me = lax.axis_index("dev")
    count, feats = owners.shape
    rows, width = table.shape
    wide = width // SPLITS
    parts = wide // LANES
    group = 1
    while group < devices and 2 * group * rows * width * 4 <= GROUP_BYTES:
        group *= 2
    columns = devices // group
    in_group = me % group
    column = me // group

    ids = (owners * rows + local_rows).T
    all_ids = [ids] + [swap(ids, k * group) for k in range(1, columns)]

    def places(v, spare):
        owner = v // rows
        place = ((owner % group) ^ in_group) * rows + v % rows
        return jnp.where(owner // group == column, place, spare) * parts

    x = []
    tabs = []
    for n in range(SPLITS):
        t = [None] * group
        t[0] = table[:, n * wide:(n + 1) * wide]
        for m in range(2, group, 2):
            t[m] = swap(t[0], m)
        tabs.append(t)
    sums = None
    for n in range(SPLITS):
        t = tabs[n]
        if sums is not None:
            sums, t = lax.optimization_barrier((sums, t))
        for m in range(0, group, 2):
            t[m + 1] = swap(t[m], 1)
        index = [places(v, group * rows).reshape(-1) for v in all_ids]
        sums = [None] * columns
        for part in (range(3, columns, 2), (*range(2, columns, 2), 1, 0)):
            kinds = [BF16 if k else F32 for k in part]
            made = gather_sum(jnp.concatenate([index[k] for k in part]), t, kinds, count)
            for k, s in zip(part, made):
                sums[k] = s
        x.append(reduce_blocks(sums, group).astype(BF16))

    out = dense(x, segments[0], weights, cotangent)
    dx, (normed, mixed, d_pre) = out[:SPLITS], out[SPLITS:]

    spare = group * rows + jnp.arange(feats, dtype=jnp.int32)[:, None]
    index = jnp.stack([places(v, spare) for v in all_ids]).reshape(-1)
    halves = []
    for n in range(SPLITS):
        pieces = gather_blocks(dx[n], columns, group, n > 0)
        outs = scatter_add(index, pieces, group, rows, (F32,) + (BF16,) * (group - 1))
        halves.append(reduce_blocks(outs, 1))
    table_grad = jnp.concatenate(halves, axis=1)

    grad_in = jnp.dot(normed.T, d_pre, preferred_element_type=F32)
    grad_out = jnp.dot(mixed.T, cotangent, preferred_element_type=F32)
    full_grad = jnp.concatenate([grad_in, grad_out], axis=1)
    grad = sum_grad(full_grad, me, group, columns, master.shape[0])
    new_m1 = 0.9 * moment1 + 0.1 * grad
    new_m2 = 0.95 * moment2 + 0.05 * grad * grad
    fix1 = 1.0 - 0.9**10
    fix2 = 1.0 - 0.95**10
    new_master = master - 0.01 * (new_m1 / fix1) / (jnp.sqrt(new_m2 / fix2) + 1e-08)
    new_weights = share_weights(new_master.astype(BF16), me, group, columns).reshape(weights.shape)
    return (table_grad, new_weights, new_master, new_m1, new_m2)


def solution(mesh):
    split = P("dev", None)
    return jax.shard_map(
        shards,
        mesh=mesh,
        in_specs=(split,) * 5 + (P(),) + (split,) * 3,
        out_specs=(split, P()) + (split,) * 3,
        check_vma=False,
    )
```

```python
import functools
import jax
import jax.numpy as jnp
from jax import lax
from jax.experimental import pallas as pl
from jax.experimental.pallas import tpu as pltpu
from jax.sharding import PartitionSpec as P

HEADS = 8
MAXLEN = 512
F32 = jnp.float32
BF16 = jnp.bfloat16
LANES = 128


def sigmoid(v):
    return 0.5 * jnp.tanh(0.5 * v) + 0.5


def nt(a, b):
    return lax.dot_general(a, b, (((1,), (1,)), ((), ())), preferred_element_type=F32)


def nn(a, b):
    return jnp.dot(a, b, preferred_element_type=F32)


def row_stats(v):
    mean = jnp.mean(v, axis=-1, keepdims=True)
    cen = v - mean
    var = jnp.mean(cen * cen, axis=-1, keepdims=True)
    rstd = lax.rsqrt(var + 1e-05)
    return cen * rstd, rstd


def norm_grad(hat, rstd, dy):
    m1 = jnp.mean(dy, axis=-1, keepdims=True)
    m2 = jnp.mean(dy * hat, axis=-1, keepdims=True)
    return rstd * (dy - m1 - hat * m2)


def dense_body(block, splits, *refs):
    x_refs, (segc_ref, segr_ref, w_ref, cot_ref) = refs[:splits], refs[splits:splits + 4]
    dx_refs, refs = refs[splits + 4:2 * splits + 4], refs[2 * splits + 4:]
    (normed_ref, mixed_ref, dpre_ref, mask, dsil, act, dmix, att, datt, wsave, dsave, dvt, dkt) = refs
    rows, width = cot_ref.shape
    wide = width // splits
    head = width // HEADS
    lanes = 2 * head
    npair = HEADS // 2
    nblk = rows // block
    band = -(-MAXLEN // block)
    tiles = [(q, k) for q in range(nblk) for k in range(max(0, q - band), q + 1)]
    where = {t: i for i, t in enumerate(tiles)}

    def rs(i):
        return pl.ds(pl.multiple_of(i * block, block), block)

    def x_rows(r):
        return jnp.concatenate([v[r, :] for v in x_refs], axis=1).astype(F32)

    def first(i, c):
        r = rs(i)
        hat, _ = row_stats(x_rows(r))
        nb = hat.astype(BF16)
        normed_ref[r, :] = nb
        for j in range(4):
            cols = slice(j * width, (j + 1) * width)
            pre = nn(nb, w_ref[:, cols])
            sg = sigmoid(pre)
            a = pre * sg
            act[r, cols] = a.astype(BF16)
            dsil[r, cols] = sg + a * (1.0 - sg)
        dmix[r, :] = nt(cot_ref[r, :], w_ref[:, 4 * width:]).astype(BF16)
        return c

    lax.fori_loop(0, nblk, first, 0)

    for j, (q, k) in enumerate(tiles):
        same = segc_ref[q * block:(q + 1) * block, :] == segr_ref[:, k * block:(k + 1) * block]
        if q == k:
            ri = lax.broadcasted_iota(jnp.int32, (block, block), 0)
            ci = lax.broadcasted_iota(jnp.int32, (block, block), 1)
            same = same & (ri >= ci)
        mask[j] = jnp.where(same, 1.0 / MAXLEN, 0.0)

    low = lax.broadcasted_iota(jnp.int32, (block, lanes), 1) < head

    def halves(v):
        zero = jnp.zeros_like(v)
        return jnp.where(low, v, zero), jnp.where(low, zero, v)

    def cols(part, p):
        return pl.ds(pl.multiple_of(part * width + p * lanes, lanes), lanes)

    def forward(p, c):
        for q in range(nblk):
            qr = slice(q * block, (q + 1) * block)
            qh = halves(act[qr, cols(2, p)])
            acc = jnp.zeros((block, lanes), F32)
            for k in range(max(0, q - band), q + 1):
                kr = slice(k * block, (k + 1) * block)
                j = where[(q, k)]
                key = act[kr, cols(3, p)]
                vh = halves(act[kr, cols(1, p)])
                for h in range(2):
                    s = nt(qh[h], key)
                    m = mask[j]
                    sg = sigmoid(s)
                    a = s * sg
                    wt = (a * m).astype(BF16)
                    wsave[p * 2 + h, j] = wt
                    dsave[p * 2 + h, j] = ((sg + a * (1.0 - sg)) * m).astype(BF16)
                    acc += nn(wt, vh[h])
            att[qr, cols(0, p)] = acc
        return c

    lax.fori_loop(0, npair, forward, 0)

    def middle(i, c):
        r = rs(i)
        hat, rstd = row_stats(att[r, :])
        g = act[r, 0:width].astype(F32)
        dm = dmix[r, :].astype(F32)
        mixed_ref[r, :] = (hat * g).astype(BF16)
        dgate = (dm * hat).astype(BF16).astype(F32)
        dpre_ref[r, 0:width] = (dgate * dsil[r, 0:width]).astype(BF16)
        datt[r, :] = norm_grad(hat, rstd, dm * g).astype(BF16)
        return c

    lax.fori_loop(0, nblk, middle, 0)

    def backward(p, c):
        dvt[...] = jnp.zeros(dvt.shape, F32)
        dkt[...] = jnp.zeros(dkt.shape, F32)
        for q in range(nblk):
            qr = slice(q * block, (q + 1) * block)
            da = datt[qr, cols(0, p)]
            qv = act[qr, cols(2, p)]
            dh = halves(da)
            dat = da.astype(F32).T.astype(BF16)
            qt = qv.astype(F32).T.astype(BF16)
            acc = jnp.zeros((block, lanes), F32)
            for k in range(max(0, q - band), q + 1):
                kr = slice(k * block, (k + 1) * block)
                j = where[(q, k)]
                val = act[kr, cols(1, p)]
                kh = halves(act[kr, cols(3, p)])
                for h in range(2):
                    hr = slice(h * head, (h + 1) * head)
                    dw = nt(dh[h], val).astype(BF16).astype(F32)
                    ds = (dw * dsave[p * 2 + h, j].astype(F32)).astype(BF16)
                    acc += nn(ds, kh[h])
                    dvt[hr, kr] += nn(dat[hr, :], wsave[p * 2 + h, j])
                    dkt[hr, kr] += nn(qt[hr, :], ds)
            dq = acc.astype(BF16).astype(F32)
            dpre_ref[qr, cols(2, p)] = (dq * dsil[qr, cols(2, p)]).astype(BF16)
        for k in range(nblk):
            kr = slice(k * block, (k + 1) * block)
            dv = dvt[:, kr].T.astype(BF16).astype(F32)
            dk = dkt[:, kr].T.astype(BF16).astype(F32)
            dpre_ref[kr, cols(1, p)] = (dv * dsil[kr, cols(1, p)]).astype(BF16)
            dpre_ref[kr, cols(3, p)] = (dk * dsil[kr, cols(3, p)]).astype(BF16)
        return c

    lax.fori_loop(0, npair, backward, 0)

    def last(i, c):
        r = rs(i)
        hat, rstd = row_stats(x_rows(r))
        dn = nt(dpre_ref[r, :], w_ref[:, 0:4 * width])
        dx = norm_grad(hat, rstd, dn) + cot_ref[r, :].astype(F32)
        for n, ref in enumerate(dx_refs):
            ref[r, :] = dx[:, n * wide:(n + 1) * wide].astype(BF16)
        return c

    lax.fori_loop(0, nblk, last, 0)


def dense(x, segs, weights, cot):
    splits = len(x)
    rows, width = cot.shape
    block = min(256, rows)
    nblk = rows // block
    band = -(-MAXLEN // block)
    ntile = sum(min(q, band) + 1 for q in range(nblk))
    lanes = 2 * width // HEADS
    vm = pl.BlockSpec(memory_space=pltpu.VMEM)
    return pl.pallas_call(
        functools.partial(dense_body, block, splits),
        out_shape=(jax.ShapeDtypeStruct((rows, width // splits), BF16),) * splits
        + (
            jax.ShapeDtypeStruct((rows, width), BF16),
            jax.ShapeDtypeStruct((rows, width), BF16),
            jax.ShapeDtypeStruct((rows, 4 * width), BF16),
        ),
        in_specs=[vm] * (splits + 4),
        out_specs=(vm,) * (splits + 3),
        scratch_shapes=[
            pltpu.VMEM((ntile, block, block), F32),
            pltpu.VMEM((rows, 4 * width), F32),
            pltpu.VMEM((rows, 4 * width), BF16),
            pltpu.VMEM((rows, width), BF16),
            pltpu.VMEM((rows, width), F32),
            pltpu.VMEM((rows, width), BF16),
            pltpu.VMEM((HEADS, ntile, block, block), BF16),
            pltpu.VMEM((HEADS, ntile, block, block), BF16),
            pltpu.VMEM((lanes, rows), F32),
            pltpu.VMEM((lanes, rows), F32),
        ],
        compiler_params=pltpu.CompilerParams(vmem_limit_bytes=60 * 1024 * 1024),
        name="dense_step",
    )(*x, segs.reshape(rows, 1), segs.reshape(1, rows), weights, cot)


def spread_rows(dst, base, src, chunk):
    rows, width = src.shape
    parts = width // LANES

    def step(i, c):
        for j in range(parts):
            piece = src[pl.ds(pl.multiple_of(i * chunk, chunk), chunk), j * LANES:(j + 1) * LANES]
            start = pl.multiple_of(base * parts + i * (chunk * parts), 8) + j
            dst[pl.ds(start, chunk, stride=parts), :] = piece.astype(F32)
        return c

    lax.fori_loop(0, rows // chunk, step, 0)


def join_rows(dst, srcs, base, chunk):
    rows, width = dst.shape
    parts = width // LANES

    def step(i, c):
        for j in range(parts):
            start = pl.multiple_of(base * parts + i * (chunk * parts), 8) + j
            piece = srcs[0][pl.ds(start, chunk, stride=parts), :]
            for src in srcs[1:]:
                piece = piece + src[pl.ds(start, chunk, stride=parts), :]
            dst[pl.ds(pl.multiple_of(i * chunk, chunk), chunk), j * LANES:(j + 1) * LANES] = piece.astype(dst.dtype)
        return c

    lax.fori_loop(0, rows // chunk, step, 0)


def gather_body(ntab, nout, unroll, idx, *refs):
    tabs, outs, tab, acc = refs[:ntab], refs[ntab:ntab + nout], refs[-2], refs[-1]
    rows, width = tabs[0].shape
    parts = width // LANES
    count = outs[0].shape[0]
    feats = idx.shape[0] // (count * nout)
    chunk = 64
    for i in range(ntab):
        spread_rows(tab, i * rows, tabs[i], chunk)
    tab[pl.ds(ntab * rows * parts, 8), :] = jnp.zeros((8, LANES), F32)
    for n, out in enumerate(outs):

        def step(i, c):
            for u in range(unroll):
                t = i * unroll + u
                total = tab[pl.ds(idx[n * feats * count + t], parts), :]
                for f in range(1, feats):
                    total = total + tab[pl.ds(idx[(n * feats + f) * count + t], parts), :]
                acc[pl.ds(t * parts, parts), :] = total
            return c

        lax.fori_loop(0, count // unroll, step, 0)
        join_rows(out, [acc], 0, chunk)


def gather_sum(idx, tabs, dtypes, count):
    rows, width = tabs[0].shape
    parts = width // LANES
    vm = pl.BlockSpec(memory_space=pltpu.VMEM)
    return pl.pallas_call(
        functools.partial(gather_body, len(tabs), len(dtypes), 8),
        out_shape=tuple(jax.ShapeDtypeStruct((count, width), d) for d in dtypes),
        in_specs=[pl.BlockSpec(memory_space=pltpu.SMEM)] + [vm] * len(tabs),
        out_specs=(vm,) * len(dtypes),
        scratch_shapes=[
            pltpu.VMEM((len(tabs) * rows * parts + 8, LANES), F32),
            pltpu.VMEM((count * parts, LANES), F32),
        ],
        compiler_params=pltpu.CompilerParams(vmem_limit_bytes=60 * 1024 * 1024),
        name="gather_sum",
    )(idx, *tabs)


def scatter_body(npiece, nout, lots, idx, *refs):
    pieces, outs, far = refs[:npiece], refs[npiece:npiece + nout // 2], refs[npiece + nout // 2]
    accs, stage = refs[npiece + nout // 2 + 1:-1], refs[-1]
    count, width = pieces[0].shape
    rows = outs[0].shape[0]
    parts = width // LANES
    feats = idx.shape[0] // (npiece * count)
    chunk = 64

    def clear(i, c):
        for acc in accs:
            acc[pl.ds(pl.multiple_of(i * 256, 256), 256), :] = jnp.zeros((256, LANES), F32)
        return c

    lax.fori_loop(0, nout * rows * parts // 256, clear, 0)
    for acc in accs:
        acc[pl.ds(nout * rows * parts, parts * feats), :] = jnp.zeros((parts * feats, LANES), F32)
    for n in range(npiece):
        spread_rows(stage, 0, pieces[n], chunk)

        def step(i, c):
            for w in range(2):
                base = (i * 2 + w) * lots
                todo = []
                for u, acc in enumerate(accs):
                    val = stage[pl.ds((base + u) * parts, parts), :]
                    for f in range(feats):
                        at = idx[(n * feats + f) * count + base + u]
                        todo.append((acc, at, acc[pl.ds(at, parts), :] + val))
                for acc, at, val in todo:
                    acc[pl.ds(at, parts), :] = val
            return c

        lax.fori_loop(0, count // (2 * lots), step, 0)
    for o in range(nout // 2):
        join_rows(outs[o], accs, 2 * o * rows, chunk)
        join_rows(far.at[o], accs, (2 * o + 1) * rows, chunk)


def scatter_add(idx, pieces, nout, rows, dtypes):
    count, width = pieces[0].shape
    feats = idx.shape[0] // (len(pieces) * count)
    parts = width // LANES
    lots = 4
    vm = pl.BlockSpec(memory_space=pltpu.VMEM)
    return pl.pallas_call(
        functools.partial(scatter_body, len(pieces), nout, lots),
        out_shape=tuple(jax.ShapeDtypeStruct((rows, width), d) for d in dtypes)
        + (jax.ShapeDtypeStruct((nout // 2, rows, width), BF16),),
        in_specs=[pl.BlockSpec(memory_space=pltpu.SMEM)] + [vm] * len(pieces),
        out_specs=(vm,) * (nout // 2 + 1),
        scratch_shapes=[pltpu.VMEM(((nout * rows + feats) * parts, LANES), F32)] * lots
        + [pltpu.VMEM((count * parts, LANES), F32)],
        compiler_params=pltpu.CompilerParams(vmem_limit_bytes=60 * 1024 * 1024),
        name="scatter_add",
    )(idx, *pieces)


def place_body(parts, at, *refs):
    blocks, out = refs[:-1], refs[-1]
    cols = blocks[0].shape[0]
    me = at[0]
    for core in range(2):
        for m in range(parts):
            ref = blocks[core * parts + m]
            for j in range(cols):
                out[(j * parts + m) * 2 + core ^ me] = ref[j]


def place_blocks(me, blocks):
    cols = blocks[0].shape[0]
    shape = (len(blocks) * cols,) + blocks[0].shape[1:]
    vm = pl.BlockSpec(memory_space=pltpu.VMEM)
    return pl.pallas_call(
        functools.partial(place_body, len(blocks) // 2),
        out_shape=jax.ShapeDtypeStruct(shape, blocks[0].dtype),
        in_specs=[pl.BlockSpec(memory_space=pltpu.SMEM)] + [vm] * len(blocks),
        out_specs=vm,
        name="place_blocks",
    )(me.reshape(1), *blocks)


SPLITS = 2
GROUP_BYTES = 16 * 1024 * 1024


def swap(v, bits):
    devices = lax.axis_size("dev")
    return lax.ppermute(v, "dev", [(i, i ^ bits) for i in range(devices)])


def gather_blocks(v, count, unit, direct):
    got = [v] + [None] * (count - 1)
    for k in range(1, count):
        mate = k % 2 and k > 1 and not direct
        got[k] = swap(got[k - 1], unit) if mate else swap(v, k * unit)
    return got


def reduce_blocks(near, far, unit):
    merged = [v.astype(F32) + f.astype(F32) for v, f in zip(near, far)]
    total = merged[0]
    for i in range(1, len(merged)):
        give = merged[i].astype(BF16)
        total = total + swap(give, 2 * i * unit).astype(F32)
    return total


def pick(v, at, axis):
    return lax.dynamic_index_in_dim(v, at, axis, keepdims=False)


def sum_grad(grad, me, group, columns, block_rows):
    half = group // 2
    v = grad.reshape(columns, half, 2, block_rows, grad.shape[1])
    core, chip, column = me % 2, me // 2 % half, me // group
    v = pick(v, core, 2) + swap(pick(v, 1 - core, 2).astype(BF16), 1).astype(F32)
    total = pick(v, chip, 1)
    for m in range(1, half):
        total = total + swap(pick(v, chip ^ m, 1).astype(BF16), 2 * m).astype(F32)
    v = total
    total = pick(v, column, 0)
    for k in range(1, columns):
        total = total + swap(pick(v, column ^ k, 0).astype(BF16), k * group).astype(F32)
    return total


def share_weights(v, me, group, columns):
    half = group // 2
    v = jnp.stack([v] + [swap(v, k * group) for k in range(1, columns)])
    near = [v] + [swap(v, 2 * m) for m in range(1, half)]
    far = [swap(n, 1) for n in near]
    return place_blocks(me, near + far)


def shards(table, owners, local_rows, segments, cotangent, weights, master, moment1, moment2):
    devices = lax.axis_size("dev")
    me = lax.axis_index("dev")
    count, feats = owners.shape
    rows, width = table.shape
    wide = width // SPLITS
    parts = wide // LANES
    group = 1
    while group < devices and 2 * group * rows * width * 4 <= GROUP_BYTES:
        group *= 2
    columns = devices // group
    in_group = me % group
    column = me // group

    ids = (owners * rows + local_rows).T
    all_ids = [ids] + [swap(ids, k * group) for k in range(1, columns)]

    def places(v, spare):
        owner = v // rows
        place = ((owner % group) ^ in_group) * rows + v % rows
        return jnp.where(owner // group == column, place, spare) * parts

    x = []
    tabs = []
    for n in range(SPLITS):
        t = [None] * group
        t[0] = table[:, n * wide:(n + 1) * wide]
        for m in range(2, group, 2):
            t[m] = swap(t[0], m)
        tabs.append(t)
    sums = None
    for n in range(SPLITS):
        t = tabs[n]
        if sums is not None:
            sums, t = lax.optimization_barrier((sums, t))
        for m in range(0, group, 2):
            t[m + 1] = swap(t[m], 1)
        index = [places(v, group * rows).reshape(-1) for v in all_ids]
        sums = [None] * columns
        for part in (range(3, columns, 2), (*range(2, columns, 2), 1, 0)):
            kinds = [BF16 if k else F32 for k in part]
            made = gather_sum(jnp.concatenate([index[k] for k in part]), t, kinds, count)
            for k, s in zip(part, made):
                sums[k] = s
        far = [swap(s, group) for s in sums[1::2]]
        x.append(reduce_blocks(sums[0::2], far, group).astype(BF16))

    out = dense(x, segments[0], weights, cotangent)
    dx, (normed, mixed, d_pre) = out[:SPLITS], out[SPLITS:]

    spare = group * rows + jnp.arange(feats, dtype=jnp.int32)[:, None]
    index = jnp.stack([places(v, spare) for v in all_ids]).reshape(-1)
    halves = []
    for n in range(SPLITS):
        pieces = gather_blocks(dx[n], columns, group, n > 0)
        outs = scatter_add(index, pieces, group, rows, (F32,) + (BF16,) * (group // 2 - 1))
        far = swap(outs[-1], 1)
        halves.append(reduce_blocks(outs[:-1], [far[i] for i in range(group // 2)], 1))
    table_grad = jnp.concatenate(halves, axis=1)

    grad_in = jnp.dot(normed.T, d_pre, preferred_element_type=F32)
    grad_out = jnp.dot(mixed.T, cotangent, preferred_element_type=F32)
    full_grad = jnp.concatenate([grad_in, grad_out], axis=1)
    grad = sum_grad(full_grad, me, group, columns, master.shape[0])
    new_m1 = 0.9 * moment1 + 0.1 * grad
    new_m2 = 0.95 * moment2 + 0.05 * grad * grad
    fix1 = 1.0 - 0.9**10
    fix2 = 1.0 - 0.95**10
    new_master = master - 0.01 * (new_m1 / fix1) / (jnp.sqrt(new_m2 / fix2) + 1e-08)
    new_weights = share_weights(new_master.astype(BF16), me, group, columns).reshape(weights.shape)
    return (table_grad, new_weights, new_master, new_m1, new_m2)


def solution(mesh):
    split = P("dev", None)
    return jax.shard_map(
        shards,
        mesh=mesh,
        in_specs=(split,) * 5 + (P(),) + (split,) * 3,
        out_specs=(split, P()) + (split,) * 3,
        check_vma=False,
    )
```
